512 devices in a mesh: space: 32 (over x, y, core), member: 16 (over z).
Axes of the slice: x: 4, y: 4, z: 16, core: 2. Of those that a mesh axis runs over, the one named last changes fastest.
Arguments:
- obs_pert: bfloat16 [80, 65536], P('member', 'space'), may hold values from -6 to 6
- innovation: bfloat16 [65536], P('space'), may hold values from -6 to 6
- obs_prec: bfloat16 [65536], P('space'), may hold values from 1 to 100
- obs_lists: int32 [6144, 256], P('space'), may hold values from 0 to 6143
- loc_weight: bfloat16 [6144, 256], P('space'), may hold values from 0.049804688 to 1
- send_rows: int32 [32, 16, 32], P('space'), may hold values from 0 to 11
- ocean_src: int32 [3072, 2], P('space'), may hold values from 0 to 511, as said below
- ocean_frac: float32 [3072], P('space'), may hold values from 0 to 1
- ocean_ens: bfloat16 [80, 3072, 2048], P(None, 'space', 'member'), may hold values from -6 to 6
Outputs:
- ocean_anal: bfloat16 [80, 3072, 2048], P(None, 'space', 'member')
The draws below stay inside these ranges and needn't reach their ends.
Inputs may be any that keep to these rules, and one draw needn't show every extreme that they name: `ocean_src`: the two slots of one ocean block differ.
All inputs are finite; a program needn't handle non-finite values.
Results may differ from the reference program's by a relative error of at most 0.0064.
Values may be sent and summed in bfloat16 or wider, within the bound.
No kernel may reach another device: no remote copies, remote signals or barrier semaphores. Data moves between devices by JAX's collectives and lax.ppermute only.
A program may use at most 64 MiB of HBM per device.

```python
import math
import jax
import jax.numpy as jnp
from jax import lax

K = 80
OBS_DEV = 2048
LOBS = 256
ABLK_TILE = 192
ITERS = 12
OB_TILE = 96
GROUP = 12
OCELLS = 2048
NOBS = 65536
ABLK = 6144
OBLK = 3072
N_SPACE = 32
N_MEMBER = 16
DEVICES = 512


def draw_ocean_src(key, part):

    def one_tile(tile_key):
        key_perm, key_order = jax.random.split(tile_key)
        shuffled = jax.random.permutation(key_perm, DEVICES)
        order = jax.random.permutation(key_order, 2 * OB_TILE)
        values = shuffled[order % DEVICES]
        return values.reshape(OB_TILE, 2)
    tile_keys = jax.random.split(jax.random.fold_in(key, 7), N_SPACE)
    return jax.vmap(one_tile)(tile_keys).reshape(OB_TILE * N_SPACE, 2).astype(jnp.int32)


def touch_ends(result, stream_key, smallest, largest):
    longest = result.shape.index(max(result.shape))
    spots = []
    for shift in (0, 1):
        where = [jax.random.randint(jax.random.fold_in(stream_key, axis), (), 0, length) for axis, length in enumerate(result.shape)]
        where[longest] = (where[longest] + shift) % result.shape[longest]
        spots.append(tuple(where))
    return result.at[spots[0]].set(smallest).at[spots[1]].set(largest)


def steps_of(stream_key, dims, shards, low, high):
    loudness, own = 1.0, jax.random.fold_in(stream_key, 6)
    for position, blocks in shards:
        draws = jnp.exp(jax.random.uniform(jax.random.fold_in(own, position), (blocks,), jnp.float32, low / len(shards), high / len(shards)))
        loudness = loudness * jnp.repeat(draws, dims[position] // blocks).reshape([-1 if axis == position else 1 for axis in range(len(dims))])
    return loudness


def noise(rng, shape, scale, reach, pieces=(), kind=jnp.bfloat16):
    result = scale * jax.random.normal(rng, shape, jnp.float32)
    if pieces:
        result = result * steps_of(rng, shape, pieces, -0.22, 0.18)
    return jnp.clip(result, -reach, reach).astype(kind)


def setup_inputs(seed: int = 0) -> dict:
    keys = jax.random.split(jax.random.key(seed), 10)
    return {
        "obs_pert": noise(keys[0], (K, NOBS), 1.0, 6.0, ((0, 16), (1, 32))),
        "innovation": noise(keys[1], (NOBS,), 1.0, 6.0, ((0, 32),)),
        "obs_prec": jnp.clip(jnp.exp(math.log(100.0) - 4.6051702 * jax.random.uniform(keys[2], (NOBS,), jnp.float32) ** steps_of(keys[2], (NOBS,), ((0, 32),), -0.2, 0.2)), 1.0, 100.0).astype(jnp.bfloat16),
        "obs_lists": touch_ends(jax.random.randint(keys[3], (ABLK, LOBS), 0, 3 * OBS_DEV), jax.random.fold_in(keys[3], 1), 0, (3 * OBS_DEV) - 1).astype(jnp.int32),
        "loc_weight": jnp.clip(0.049804688 + 0.9501953 * jax.random.uniform(keys[4], (ABLK, LOBS), jnp.float32) ** steps_of(keys[4], (ABLK, LOBS), ((0, 32),), -0.2, 0.2), 0.049804688, 1.0).astype(jnp.bfloat16),
        "send_rows": touch_ends(jax.random.randint(keys[5], (N_SPACE, N_MEMBER, N_SPACE), 0, GROUP), jax.random.fold_in(keys[5], 1), 0, GROUP - 1).astype(jnp.int32),
        "ocean_src": draw_ocean_src(jax.random.fold_in(keys[9], 71), 0),
        "ocean_frac": jnp.clip(1.0 * jax.random.uniform(keys[7], (OBLK,), jnp.float32) ** steps_of(keys[7], (OBLK,), ((0, 32),), -0.2, 0.2), 0.0, 1.0),
        "ocean_ens": noise(keys[8], (K, OBLK, OCELLS), 1.0, 6.0, ((1, 32), (2, 16))),
    }


def transform(local_obs, loc_sel, innov_sel, prec_sel):
    members = local_obs.shape[0]
    obs_f32 = local_obs.astype(jnp.float32)
    obs_weight = loc_sel.astype(jnp.float32) * prec_sel.astype(jnp.float32)
    weighted = obs_f32 * obs_weight[None]
    gram = jnp.einsum('ibl,jbl->bij', weighted, obs_f32, precision=lax.Precision.HIGHEST)
    pulled = jnp.einsum('ibl,bl->bi', weighted, innov_sel.astype(jnp.float32), precision=lax.Precision.HIGHEST)
    identity = jnp.eye(members, dtype=jnp.float32)
    precision_mat = (members - 1.0) * identity + gram
    scale_sum = jnp.trace(precision_mat, axis1=1, axis2=2)
    root_start = precision_mat / scale_sum[:, None, None]
    inverse_start = jnp.broadcast_to(identity, precision_mat.shape)

    def newton(iteration, carry):
        root_iter, inverse_iter = carry
        correction = 1.5 * identity - 0.5 * jnp.einsum('bij,bjk->bik', inverse_iter, root_iter, precision=lax.Precision.HIGHEST)
        root_next = jnp.einsum('bij,bjk->bik', root_iter, correction, precision=lax.Precision.HIGHEST)
        inverse_next = jnp.einsum('bij,bjk->bik', correction, inverse_iter, precision=lax.Precision.HIGHEST)
        return (root_next, inverse_next)
    root_iter, inverse_iter = lax.fori_loop(0, ITERS, newton, (root_start, inverse_start))
    spread = jnp.sqrt((members - 1.0) / scale_sum)[:, None, None] * inverse_iter
    half_way = jnp.einsum('bij,bj->bi', inverse_iter, pulled, precision=lax.Precision.HIGHEST)
    mean_weight = jnp.einsum('bij,bj->bi', inverse_iter, half_way, precision=lax.Precision.HIGHEST) / scale_sum[:, None]
    return (spread + mean_weight[:, :, None]).astype(jnp.bfloat16)

def apply_weights(ensemble, trans_one, trans_two, frac):
    frac_col = frac[:, None, None]
    mixed = ((1.0 - frac_col) * trans_one.astype(jnp.float32) + frac_col * trans_two.astype(jnp.float32)).astype(jnp.bfloat16)
    ens_f32 = ensemble.astype(jnp.float32)
    ens_mean = lax.optimization_barrier(jnp.mean(ens_f32, axis=0))
    deviation = (ens_f32 - ens_mean[None]).astype(jnp.bfloat16)
    product = jnp.einsum('jol,oji->iol', deviation.astype(jnp.float32), mixed.astype(jnp.float32))
    return (ens_mean[None] + product).astype(jnp.bfloat16)

def reference(obs_pert, innovation, obs_prec, obs_lists, loc_weight, send_rows, ocean_src, ocean_frac, ocean_ens):
    group_len = ABLK_TILE // N_MEMBER
    total_obs = obs_pert.shape[1]

    def one_tile(tile_idx):
        sources = lax.dynamic_slice_in_dim(ocean_src, tile_idx * OB_TILE, OB_TILE, 0).reshape(-1)
        member_part = sources // N_SPACE
        space_part = sources % N_SPACE
        local_row = send_rows[space_part, member_part, tile_idx]
        block_ids = (space_part * ABLK_TILE + member_part * group_len + local_row).astype(jnp.int32)
        lists = obs_lists[block_ids]
        offsets = (space_part - 1) * OBS_DEV
        global_idx = ((lists + offsets[:, None]) % total_obs).astype(jnp.int32)
        local_obs = obs_pert[:, global_idx]
        weights = transform(local_obs, loc_weight[block_ids], innovation[global_idx], obs_prec[global_idx])
        weights = weights.reshape(OB_TILE, 2, K, K)
        ensemble = lax.dynamic_slice_in_dim(ocean_ens, tile_idx * OB_TILE, OB_TILE, 1)
        frac = lax.dynamic_slice_in_dim(ocean_frac, tile_idx * OB_TILE, OB_TILE, 0)
        return apply_weights(ensemble, weights[:, 0], weights[:, 1], frac)
    tiles = lax.map(one_tile, jnp.arange(N_SPACE, dtype=jnp.int32))
    return jnp.moveaxis(tiles, 0, 1).reshape(K, OB_TILE * N_SPACE, OCELLS)
```

```python
import jax
import jax.numpy as jnp
from jax import lax
from jax.experimental import pallas as pl
from jax.experimental.pallas import tpu as pltpu
from jax.sharding import PartitionSpec as P

ITERS = 12
LANES = 128
HALF = 16


def iota2(shape, dim):
    return lax.broadcasted_iota(jnp.int32, shape, dim)


def split(x):
    high = x.astype(jnp.bfloat16)
    low = (x - high.astype(jnp.float32)).astype(jnp.bfloat16)
    return high, low


def mm(x, y):
    (xh, xl), (yh, yl) = x, y
    dot = lambda a, b: jnp.dot(a, b, preferred_element_type=jnp.float32)
    return dot(xh, yl) + dot(xl, yh) + dot(xh, yh)


def transform_body(
    lists, loc, left, own, right, out, table, rows, rh, rl, zh, zl, mh, ml, side, wide, packed, packed2
):
    group, local = lists.shape
    tile = own.shape[0]
    members = rh.shape[1]
    for i, part in enumerate((left, own, right)):
        table[pl.ds(i * tile, tile), :] = part[...].astype(jnp.float32)
    eye = (iota2((members, members), 0) == iota2((members, members), 1)).astype(jnp.float32)
    step = 16

    for a in range(group):

        def pull(i, carry, a=a):
            for u in range(step):
                spot = lists[a, i * step + u]
                rows[a, pl.ds(i * step + u, 1), :] = table[pl.ds(spot, 1), :]
            return carry

        lax.fori_loop(0, local // step, pull, 0)
    for a in range(group):
        y = rows[a]
        weight = loc[:, a : a + 1] * y[:, members + 1 : members + 2]
        high, low = split(y * weight)
        y16 = y.astype(jnp.bfloat16)
        dims = (((0,), (0,)), ((), ()))
        gram = lax.dot_general(y16, low, dims, preferred_element_type=jnp.float32)
        gram += lax.dot_general(y16, high, dims, preferred_element_type=jnp.float32)
        mat = gram[:members, :members] + (members - 1.0) * eye
        trace = jnp.sum(
            jnp.sum(mat * eye, axis=1, keepdims=True), axis=0, keepdims=True
        )
        side[a, 0:1, :] = gram[members : members + 1, :]
        side[a, 1:2, :] = jnp.broadcast_to(trace, (1, LANES))
        start = mat / trace
        r = split(start)
        m = split(1.5 * eye - 0.5 * start)
        rh[a], rl[a] = split(mm(r, m))
        zh[a], zl[a] = m

    def newton(i, carry):
        for a in range(group):
            corr = 1.5 * eye - 0.5 * mm((zh[a], zl[a]), (rh[a], rl[a]))
            mh[a], ml[a] = split(corr)
        for a in range(group):
            m = (mh[a], ml[a])
            rh[a], rl[a] = split(mm((rh[a], rl[a]), m))
            zh[a], zl[a] = split(mm(m, (zh[a], zl[a])))
        return carry

    lax.fori_loop(0, ITERS - 2, newton, 0)
    packed[...] = jnp.zeros(packed.shape, jnp.float32)
    packed2[...] = jnp.zeros(packed.shape, jnp.float32)
    lane = iota2((2 * HALF, LANES), 1)
    row = iota2((HALF, LANES), 0)
    for a in range(group):
        z = (zh[a], zl[a])
        corr = 1.5 * eye - 0.5 * mm(z, (rh[a], rl[a]))
        inverse = mm(split(corr), z)
        trace = side[a, 1:2, :members]
        pulled = side[a, 0:1, :members]
        half_way = jnp.sum(inverse * pulled, axis=1, keepdims=True)
        mean_weight = jnp.sum(inverse * half_way, axis=0, keepdims=True) / trace
        wide[0:members, 0:members] = inverse * jnp.sqrt((members - 1.0) / trace)
        wide[members : members + 1, 0:members] = mean_weight
        body = jnp.where(lane < 80, wide[48:80, :], pltpu.roll(wide[16:48, :], 80, 1))
        corner = pltpu.roll(wide[0:16, :], 64, 1)
        mean_rows = jnp.broadcast_to(wide[80:81, :], (HALF, LANES))
        lane_top = lane[:HALF]
        top = jnp.where((lane_top >= 64) & (lane_top < 80), corner, body[:HALF])
        for k in range(5):
            moved = pltpu.roll(mean_rows, 112 - 16 * k, 1)
            top = jnp.where((lane_top >= 112) & (row == k), moved, top)
        packed[pl.ds(a, HALF, stride=16), :] = top
        packed2[pl.ds(a, HALF, stride=16), :] = body[HALF:]
    out[:, 0:LANES] = packed[...].astype(jnp.bfloat16)
    out[:, LANES : 2 * LANES] = packed2[...].astype(jnp.bfloat16)


def transforms(lists, loc_cols, left, own, right, members):
    group, local = lists.shape
    tile = own.shape[0]
    f32, b16 = jnp.float32, jnp.bfloat16
    vmem = pl.BlockSpec(memory_space=pltpu.VMEM)
    small = (group, members, members)
    return pl.pallas_call(
        transform_body,
        out_shape=jax.ShapeDtypeStruct((16 * 16, 2 * LANES), b16),
        in_specs=[pl.BlockSpec(memory_space=pltpu.SMEM), vmem, vmem, vmem, vmem],
        out_specs=vmem,
        scratch_shapes=[
            pltpu.VMEM((3 * tile, LANES), f32),
            pltpu.VMEM((group, local, LANES), f32),
            pltpu.VMEM(small, b16),
            pltpu.VMEM(small, b16),
            pltpu.VMEM(small, b16),
            pltpu.VMEM(small, b16),
            pltpu.VMEM(small, b16),
            pltpu.VMEM(small, b16),
            pltpu.VMEM((group, 8, LANES), f32),
            pltpu.VMEM((88, LANES), f32),
            pltpu.VMEM((16 * 16, LANES), f32),
            pltpu.VMEM((16 * 16, LANES), f32),
        ],
        name="transforms",
    )(lists, loc_cols, left, own, right)


def apply_body(pieces, ens, out, ens32, mix32, mix32b, out32):
    members, blocks = ens.shape[0], ens.shape[1]
    wide = ens[...].astype(jnp.float32)
    mean = jnp.sum(wide, axis=0) * (1.0 / members)
    ens32[...] = wide.reshape(members * blocks, LANES)
    mix32[...] = pieces[:, :, 0:LANES].astype(jnp.float32).reshape(16 * blocks, LANES)
    mix32b[...] = pieces[:, :, LANES:].astype(jnp.float32).reshape(16 * blocks, LANES)
    lane = iota2((members, LANES), 1)
    row = iota2((members, LANES), 0)
    lane8 = iota2((8, LANES), 1)
    row8 = iota2((8, LANES), 0)
    for o in range(blocks):
        first = mix32[pl.ds(o, 16, stride=blocks), :]
        second = mix32b[pl.ds(o, 16, stride=blocks), :]
        pack = jnp.concatenate([first, second], axis=0)
        flip = jnp.transpose(jnp.concatenate([pack, jnp.zeros((96, LANES), jnp.float32)], axis=0))
        lower = jnp.concatenate(
            [pltpu.roll(first, 64, 1), pltpu.roll(pack, 48, 1), pack], axis=0
        )
        right = pltpu.roll(flip[:80], 48, 1)
        inner = pltpu.roll(flip[80:], 16, 1)
        upper = jnp.concatenate(
            [jnp.where(lane[:48] < 48, inner, right[:48]), right[48:]], axis=0
        )
        spread = jnp.where((lane <= row) | (lane < 16), lower, upper)
        means = pltpu.roll(first[:8], 16, 1, stride=16, stride_axis=0)
        means = jnp.where(lane8 // 16 == row8, means, 0.0)
        means = jnp.sum(means, axis=0, keepdims=True)
        weights = (spread + means).astype(jnp.bfloat16)[:, :members]
        base = mean[o : o + 1, :]
        dev = (ens32[pl.ds(o, members, stride=blocks), :] - base).astype(jnp.bfloat16)
        product = jnp.dot(weights, dev, preferred_element_type=jnp.float32)
        out32[pl.ds(o, members, stride=blocks), :] = base + product
    out[...] = out32[...].reshape(members, blocks, LANES).astype(jnp.bfloat16)


def apply_weights(pieces, ensemble):
    members, blocks, cells = ensemble.shape
    step = 16
    f32 = jnp.float32
    return pl.pallas_call(
        apply_body,
        grid=(blocks // step,),
        out_shape=jax.ShapeDtypeStruct(ensemble.shape, jnp.bfloat16),
        in_specs=[
            pl.BlockSpec((16, step, 2 * LANES), lambda i: (0, i, 0)),
            pl.BlockSpec((members, step, cells), lambda i: (0, i, 0)),
        ],
        out_specs=pl.BlockSpec((members, step, cells), lambda i: (0, i, 0)),
        scratch_shapes=[
            pltpu.VMEM((members * step, LANES), f32),
            pltpu.VMEM((16 * step, LANES), f32),
            pltpu.VMEM((16 * step, LANES), f32),
            pltpu.VMEM((members * step, LANES), f32),
        ],
        name="apply",
    )(pieces, ensemble)


def shards(
    obs_pert,
    innovation,
    obs_prec,
    obs_lists,
    loc_weight,
    send_rows,
    ocean_src,
    ocean_frac,
    ocean_ens,
):
    n_member = lax.axis_size("member")
    n_space = lax.axis_size("space")
    member_idx = lax.axis_index("member")
    own_members, tile_obs = obs_pert.shape
    members = own_members * n_member
    chunks = tile_obs // LANES
    b16 = jnp.bfloat16

    flat = obs_pert.reshape(own_members * chunks, LANES)
    spread = lax.all_to_all(
        jnp.broadcast_to(flat[None], (n_member, *flat.shape)), "member", 0, 0, tiled=True
    )
    by_obs = spread.reshape(n_member, own_members, chunks, LANES).transpose(2, 3, 0, 1)
    by_obs = by_obs.reshape(tile_obs, members)
    own = jnp.concatenate(
        [
            by_obs,
            innovation[:, None],
            obs_prec[:, None],
            jnp.zeros((tile_obs, LANES - members - 2), b16),
        ],
        axis=1,
    )
    left = lax.ppermute(own, "space", [(i, (i + 1) % n_space) for i in range(n_space)])
    right = lax.ppermute(own, "space", [((i + 1) % n_space, i) for i in range(n_space)])

    group = obs_lists.shape[0] // n_member
    lists_mine = lax.dynamic_slice_in_dim(obs_lists, member_idx * group, group, 0)
    loc_mine = lax.dynamic_slice_in_dim(loc_weight, member_idx * group, group, 0)
    loc_cols = loc_mine.astype(jnp.float32).T
    pieces = transforms(lists_mine, loc_cols, left, own, right, members)

    arrived_one = lax.all_to_all(
        pieces.reshape(n_member, 16, 2 * LANES), "member", 0, 0, tiled=True
    ).reshape(n_member * 16, 2 * LANES)
    choice = (send_rows[0] + 16 * jnp.arange(n_member, dtype=jnp.int32)[:, None]).T.reshape(-1)
    pick = (choice[:, None] == jnp.arange(n_member * 16, dtype=jnp.int32)[None]).astype(b16)
    chosen = jnp.dot(pick, arrived_one, preferred_element_type=jnp.float32).astype(b16)
    arrived = lax.all_to_all(
        chosen.reshape(n_space, n_member, 2 * LANES), "space", 0, 0, tiled=True
    ).reshape(n_space * n_member, 2 * LANES)
    slot = (ocean_src % n_space) * n_member + ocean_src // n_space
    places = jnp.arange(n_space * n_member, dtype=jnp.int32)[None]
    frac = ocean_frac[:, None]
    coef = jnp.where(slot[:, :1] == places, 1.0 - frac, 0.0) + jnp.where(
        slot[:, 1:] == places, frac, 0.0
    )
    mixed = jnp.dot(
        coef, arrived.astype(jnp.float32), precision=lax.Precision.HIGHEST
    ).astype(b16)
    everything = lax.all_gather(mixed, "member", axis=0, tiled=False)
    return apply_weights(everything, ocean_ens)


def solution(mesh):
    return jax.shard_map(
        shards,
        mesh=mesh,
        in_specs=(
            P("member", "space"),
            P("space"),
            P("space"),
            P("space", None),
            P("space", None),
            P("space", None, None),
            P("space", None),
            P("space"),
            P(None, "space", "member"),
        ),
        out_specs=P(None, "space", "member"),
        check_vma=False,
    )
```

```python
import jax
import jax.numpy as jnp
from jax import lax
from jax.experimental import pallas as pl
from jax.experimental.pallas import tpu as pltpu
from jax.sharding import PartitionSpec as P

ITERS = 12
LANES = 128
HALF = 16


def iota2(shape, dim):
    return lax.broadcasted_iota(jnp.int32, shape, dim)


def split(x):
    high = x.astype(jnp.bfloat16)
    low = (x - high.astype(jnp.float32)).astype(jnp.bfloat16)
    return high, low


def as_left(x):
    lane = iota2(x.shape, 1)
    high = x.astype(jnp.bfloat16).astype(jnp.float32)
    low = pltpu.roll(x - high, 80, 1)
    again = pltpu.roll(high, 32, 1)
    first = jnp.where(lane < 80, high, low)
    second = jnp.where(lane < 32, low, again)
    return jnp.concatenate([first.astype(jnp.bfloat16), second.astype(jnp.bfloat16)], axis=1)


def as_right(x):
    high, low = split(x)
    return jnp.concatenate([high, high, low, jnp.zeros((16, x.shape[1]), jnp.bfloat16)], axis=0)


def product(left, right):
    return jnp.dot(left, right, preferred_element_type=jnp.float32)


def transform_body(
    lists, loc, left, own, right, out, table, rows, rl, rr, zl, zr, ml, mr, side, packed
):
    group, local = loc.shape
    tile = own.shape[0]
    members = rl.shape[1]
    for i, part in enumerate((left, own, right)):
        table[pl.ds(i * tile, tile), :] = part[...].astype(jnp.float32)
    eye = (iota2((members, LANES), 0) == iota2((members, LANES), 1)).astype(jnp.float32)
    inside = iota2((members, LANES), 1) < members
    step = 32
    batch = 4

    def pull(i, carry):
        for u in range(step):
            spot = lists[i * step + u]
            rows[pl.ds(i * step + u, 1), :] = table[pl.ds(spot, 1), :]
        return carry

    lax.fori_loop(0, group * local // step, pull, 0)

    def begin(i, carry):
        for k in range(batch):
            a = i * batch + k
            y = rows[pl.ds(a * local, local), :]
            turned = jnp.transpose(y)[:88]
            weight = loc[pl.ds(a, 1), :] * turned[members + 1 : members + 2]
            high, low = split(turned * weight)
            y16 = y.astype(jnp.bfloat16)
            gram = product(low, y16) + product(high, y16)
            mat = jnp.where(inside, gram[:members], 0.0) + (members - 1.0) * eye
            trace = jnp.sum(
                jnp.sum(mat * eye, axis=0, keepdims=True), axis=1, keepdims=True
            )
            side[a, 0:1, :] = gram[members : members + 1, :]
            side[a, 1:2, :] = jnp.broadcast_to(trace, (1, LANES))
            start = mat / trace
            corr = 1.5 * eye - 0.5 * start
            right = as_right(corr)
            zl[a], zr[a] = as_left(corr), right
            root = product(as_left(start), right)
            rl[a], rr[a] = as_left(root), as_right(root)
        return carry

    lax.fori_loop(0, group // batch, begin, 0)

    def newton(i, carry):
        for a in range(group):
            corr = 1.5 * eye - 0.5 * product(zl[a], rr[a])
            ml[a], mr[a] = as_left(corr), as_right(corr)
        for a in range(group):
            root = product(rl[a], mr[a])
            inverse = product(ml[a], zr[a])
            rl[a], rr[a] = as_left(root), as_right(root)
            zl[a], zr[a] = as_left(inverse), as_right(inverse)
        return carry

    lax.fori_loop(0, ITERS - 2, newton, 0)
    lane = iota2((2 * HALF, LANES), 1)
    row8 = iota2((8, LANES), 0)

    def finish(i, carry):
        for k in range(batch):
            a = i * batch + k
            corr = 1.5 * eye - 0.5 * product(zl[a], rr[a])
            inverse = product(as_left(corr), zr[a])
            trace = side[a, 1:2, :]
            half_way = jnp.sum(
                jnp.where(inside, inverse * side[a, 0:1, :], 0.0), axis=1, keepdims=True
            )
            mean_weight = jnp.sum(inverse * half_way, axis=0, keepdims=True) / trace
            spread = inverse * jnp.sqrt((members - 1.0) / trace)
            body = jnp.where(lane < 80, spread[48:80], pltpu.roll(spread[16:48], 80, 1))
            corner = pltpu.roll(spread[0:16], 64, 1)
            mean_rows = jnp.broadcast_to(mean_weight, (8, LANES))
            moved = jnp.zeros((8, LANES), jnp.float32)
            for p in range(5):
                moved = jnp.where(row8 == p, pltpu.roll(mean_rows, 112 - 16 * p, 1), moved)
            lane_top = lane[:HALF]
            top = jnp.where((lane_top >= 64) & (lane_top < 80), corner, body[:HALF])
            mean_top = jnp.where((lane[:8] >= 112) & (row8 < 5), moved, top[:8])
            top = jnp.concatenate([mean_top, top[8:]], axis=0)
            packed[pl.ds(a, HALF, stride=2 * group), :] = top
            packed[pl.ds(group + a, HALF, stride=2 * group), :] = body[HALF:]
        return carry

    lax.fori_loop(0, group // batch, finish, 0)
    out[...] = packed[...].astype(jnp.bfloat16)


def transforms(lists, loc, left, own, right, members):
    group, local = loc.shape
    lists = lists.reshape(-1)
    tile = own.shape[0]
    f32, b16 = jnp.float32, jnp.bfloat16
    vmem = pl.BlockSpec(memory_space=pltpu.VMEM)
    low_high = pltpu.VMEM((group, members, 2 * LANES), b16)
    stacked = pltpu.VMEM((group, 2 * LANES, LANES), b16)
    return pl.pallas_call(
        transform_body,
        out_shape=jax.ShapeDtypeStruct((HALF * 2 * group, LANES), b16),
        in_specs=[pl.BlockSpec(memory_space=pltpu.SMEM), vmem, vmem, vmem, vmem],
        out_specs=vmem,
        scratch_shapes=[
            pltpu.VMEM((3 * tile, LANES), f32),
            pltpu.VMEM((group * local, LANES), f32),
            low_high,
            stacked,
            low_high,
            stacked,
            low_high,
            stacked,
            pltpu.VMEM((group, 8, LANES), f32),
            pltpu.VMEM((HALF * 2 * group, LANES), f32),
        ],
        name="transforms",
    )(lists, loc, left, own, right)


def deviation_body(ens, dev, mean, ens32):
    members, blocks = ens.shape[0], ens.shape[1]
    wide = ens[...].astype(jnp.float32)
    center = jnp.sum(wide, axis=0) * (1.0 / members)
    mean[...] = center
    ens32[...] = (wide - center[None]).reshape(members * blocks, LANES)
    for o in range(blocks):
        dev[o] = ens32[pl.ds(o, members, stride=blocks), :].astype(jnp.bfloat16)


def deviations(ensemble):
    members, blocks, cells = ensemble.shape
    step = 16
    return pl.pallas_call(
        deviation_body,
        grid=(blocks // step,),
        out_shape=(
            jax.ShapeDtypeStruct((blocks, members, cells), jnp.bfloat16),
            jax.ShapeDtypeStruct((blocks, cells), jnp.float32),
        ),
        in_specs=[pl.BlockSpec((members, step, cells), lambda i: (0, i, 0))],
        out_specs=(
            pl.BlockSpec((step, members, cells), lambda i: (i, 0, 0)),
            pl.BlockSpec((step, cells), lambda i: (i, 0)),
        ),
        scratch_shapes=[pltpu.VMEM((members * step, LANES), jnp.float32)],
        name="deviations",
    )(ensemble)


def apply_body(pieces, pieces2, dev, mean, out, mix32, mix32b, out32):
    members, blocks = out.shape[0], out.shape[1]
    mix32[...] = pieces[...].astype(jnp.float32).reshape(16 * blocks, LANES)
    mix32b[...] = pieces2[...].astype(jnp.float32).reshape(16 * blocks, LANES)
    lane = iota2((16, LANES), 1)
    row = iota2((16, LANES), 0)
    lane8, row8 = lane[:8], row[:8]
    zero = jnp.zeros((16, LANES), jnp.float32)
    none = jnp.zeros((16, LANES), jnp.bfloat16)
    keep = lambda low, high, x: jnp.where((lane >= low) & (lane < high), x, 0.0)

    for g in range(blocks // 4):
        packs = []
        for k in range(4):
            packs.append(mix32[pl.ds(4 * g + k, 16, stride=blocks), :])
            packs.append(mix32b[pl.ds(4 * g + k, 16, stride=blocks), :])
        flip = jnp.transpose(jnp.concatenate(packs, axis=0))
        for k in range(4):
            o = 4 * g + k
            first, second = packs[2 * k], packs[2 * k + 1]
            at = 32 * k
            inner_at = (32, 0, 32, 0)[k]
            corner_at = (64, 64, 96, 64)[k]
            inner = pltpu.roll(flip[80:112], (inner_at - at) % LANES, 1)
            corner = pltpu.roll(first, 32, 1) if corner_at == 96 else first
            means = pltpu.roll(first[:8], 16, 1, stride=16, stride_axis=0)
            means = jnp.where((lane8 // 16 == row8) & (row8 < 5), means, 0.0)
            means = jnp.sum(means, axis=0, keepdims=True)
            means = jnp.where(row == 0, jnp.broadcast_to(means, row.shape), 0.0)
            direct = [
                zero,
                keep(80, 112, first),
                keep(80, 128, second[:16]),
                keep(0, 64, first),
                keep(0, 80, second),
                means,
            ]
            turned = [
                keep(at, at + 32, flip[0:16])
                + keep(inner_at, inner_at + 32, inner[:16])
                + keep(corner_at, corner_at + 16, corner),
                keep(at, at + 32, flip[16:32]) + keep(inner_at + 16, inner_at + 32, inner[16:]),
                keep(at, at + 32, flip[32:48]),
                keep(at + 16, at + 32, flip[48:64]),
                zero,
                zero,
            ]
            weights = jnp.concatenate(
                [
                    jnp.concatenate(direct, axis=0).astype(jnp.bfloat16),
                    jnp.concatenate(turned, axis=0).astype(jnp.bfloat16),
                ],
                axis=1,
            )
            d = dev[o]
            outer, middle, start = d[48:80], d[16:48], d[0:16]
            tail = (
                [outer, middle, start, none, none, none],
                [middle, outer, start, none, none, none],
                [none, none, middle, outer, start, none],
                [middle, none, none, start, none, outer],
            )[k]
            source = jnp.concatenate([d, d[:48]] + tail, axis=0)
            result = jnp.dot(weights, source, preferred_element_type=jnp.float32)
            base = mean[o : o + 1, :] + result[members : members + 1]
            out32[pl.ds(o, members, stride=blocks), :] = result[:members] + base
    out[...] = out32[...].reshape(members, blocks, LANES).astype(jnp.bfloat16)


def apply_weights(pieces, dev, mean):
    blocks, members, cells = dev.shape
    step = 16
    f32 = jnp.float32
    return pl.pallas_call(
        apply_body,
        grid=(blocks // step,),
        out_shape=jax.ShapeDtypeStruct((members, blocks, cells), jnp.bfloat16),
        in_specs=[
            pl.BlockSpec((16, step, LANES), lambda i: (0, i, 0)),
            pl.BlockSpec((16, step, LANES), lambda i: (0, blocks // step + i, 0)),
            pl.BlockSpec((step, members, cells), lambda i: (i, 0, 0)),
            pl.BlockSpec((step, cells), lambda i: (i, 0)),
        ],
        out_specs=pl.BlockSpec((members, step, cells), lambda i: (0, i, 0)),
        scratch_shapes=[
            pltpu.VMEM((16 * step, LANES), f32),
            pltpu.VMEM((16 * step, LANES), f32),
            pltpu.VMEM((members * step, LANES), f32),
        ],
        name="apply",
    )(pieces, pieces, dev, mean)


def shards(
    obs_pert,
    innovation,
    obs_prec,
    obs_lists,
    loc_weight,
    send_rows,
    ocean_src,
    ocean_frac,
    ocean_ens,
):
    n_member = lax.axis_size("member")
    n_space = lax.axis_size("space")
    member_idx = lax.axis_index("member")
    own_members, tile_obs = obs_pert.shape
    members = own_members * n_member
    chunks = tile_obs // LANES
    b16 = jnp.bfloat16

    flat = obs_pert.reshape(own_members * chunks, LANES)
    spread = lax.all_to_all(
        jnp.broadcast_to(flat[None], (n_member, *flat.shape)), "member", 0, 0, tiled=True
    )
    spread, innovation, obs_prec, obs_lists, loc_weight, send_rows, ocean_ens = (
        lax.optimization_barrier(
            (spread, innovation, obs_prec, obs_lists, loc_weight, send_rows, ocean_ens)
        )
    )
    by_obs = spread.reshape(n_member, own_members, chunks, LANES).transpose(2, 3, 0, 1)
    by_obs = by_obs.reshape(tile_obs, members)
    own = jnp.concatenate(
        [
            by_obs,
            innovation[:, None],
            obs_prec[:, None],
            jnp.zeros((tile_obs, LANES - members - 2), b16),
        ],
        axis=1,
    )
    left = lax.ppermute(own, "space", [(i, (i + 1) % n_space) for i in range(n_space)])
    right = lax.ppermute(own, "space", [((i + 1) % n_space, i) for i in range(n_space)])

    group = obs_lists.shape[0] // n_member
    lists_mine = lax.dynamic_slice_in_dim(obs_lists, member_idx * group, group, 0)
    loc_mine = lax.dynamic_slice_in_dim(loc_weight, member_idx * group, group, 0)
    loc_mine = loc_mine.astype(jnp.float32)
    count = 2 * n_member
    home = jnp.arange(n_member, dtype=jnp.int32)[:, None] * (2 * group)
    choice = (send_rows[0] + home).T
    choice = jnp.concatenate([choice, choice + group], axis=1).reshape(-1)
    dev, mean = deviations(ocean_ens)
    lists_mine, loc_mine, left, own, right, choice, dev, mean = lax.optimization_barrier(
        (lists_mine, loc_mine, left, own, right, choice, dev, mean)
    )
    pieces = transforms(lists_mine, loc_mine, left, own, right, members)

    arrived_one = lax.all_to_all(
        pieces.reshape(n_member, 2 * group, LANES), "member", 0, 0, tiled=True
    ).reshape(n_member * 2 * group, LANES)
    arrived_one, ocean_src, ocean_frac = lax.optimization_barrier(
        (arrived_one, ocean_src, ocean_frac)
    )
    places = jnp.arange(n_member * 2 * group, dtype=jnp.int32)[None]
    pick = (choice[:, None] == places).astype(b16)
    chosen = jnp.dot(pick, arrived_one, preferred_element_type=jnp.float32).astype(b16)
    arrived = lax.all_to_all(
        chosen.reshape(n_space, count, LANES), "space", 0, 0, tiled=True
    ).reshape(n_space * count, LANES)
    slot = (ocean_src % n_space) * count + ocean_src // n_space
    slot = jnp.concatenate([slot, slot + n_member], axis=0)
    frac = jnp.concatenate([ocean_frac, ocean_frac])[:, None]
    places = jnp.arange(n_space * count, dtype=jnp.int32)[None]
    coef = jnp.where(slot[:, :1] == places, 1.0 - frac, 0.0) + jnp.where(
        slot[:, 1:] == places, frac, 0.0
    )
    halves = jnp.dot(
        coef, arrived.astype(jnp.float32), precision=lax.Precision.HIGHEST
    ).astype(b16)
    everything = lax.all_gather(halves, "member", axis=0, tiled=True)
    return apply_weights(everything.reshape(n_member, *halves.shape), dev, mean)


def solution(mesh):
    return jax.shard_map(
        shards,
        mesh=mesh,
        in_specs=(
            P("member", "space"),
            P("space"),
            P("space"),
            P("space", None),
            P("space", None),
            P("space", None, None),
            P("space", None),
            P("space"),
            P(None, "space", "member"),
        ),
        out_specs=P(None, "space", "member"),
        check_vma=False,
    )
```

```python
import jax
import jax.numpy as jnp
from jax import lax
from jax.experimental import pallas as pl
from jax.experimental.pallas import tpu as pltpu
from jax.sharding import PartitionSpec as P

ITERS = 12
LANES = 128
HALF = 16


def in_vmem(x):
    return pltpu.with_memory_space_constraint(x, pltpu.VMEM)


def iota2(shape, dim):
    return lax.broadcasted_iota(jnp.int32, shape, dim)


def split(x):
    high = x.astype(jnp.bfloat16)
    low = (x - high.astype(jnp.float32)).astype(jnp.bfloat16)
    return high, low


def as_left(x):
    lane = iota2(x.shape, 1)
    high = x.astype(jnp.bfloat16).astype(jnp.float32)
    low = pltpu.roll(x - high, 80, 1)
    again = pltpu.roll(high, 32, 1)
    first = jnp.where(lane < 80, high, low)
    second = jnp.where(lane < 32, low, again)
    return jnp.concatenate([first.astype(jnp.bfloat16), second.astype(jnp.bfloat16)], axis=1)


def as_right(x):
    high, low = split(x)
    return jnp.concatenate([high, high, low, jnp.zeros((16, x.shape[1]), jnp.bfloat16)], axis=0)


def product(left, right):
    return jnp.dot(left, right, preferred_element_type=jnp.float32)


def transform_body(
    lists, loc, left, own, right, out, table, rows, rl, rr, zl, zr, ml, mr, side, packed
):
    group, local = loc.shape
    tile = own.shape[0]
    members = rl.shape[1]
    for i, part in enumerate((left, own, right)):
        table[pl.ds(i * tile, tile), :] = part[...].astype(jnp.float32)
    eye = (iota2((members, LANES), 0) == iota2((members, LANES), 1)).astype(jnp.float32)
    inside = iota2((members, LANES), 1) < members
    step = 32
    batch = 4

    def pull(i, carry):
        for u in range(step):
            spot = lists[i * step + u]
            rows[pl.ds(i * step + u, 1), :] = table[pl.ds(spot, 1), :]
        return carry

    lax.fori_loop(0, group * local // step, pull, 0)

    def begin(i, carry):
        for k in range(batch):
            a = i * batch + k
            y = rows[pl.ds(a * local, local), :]
            turned = jnp.transpose(y.astype(jnp.bfloat16))[:96].astype(jnp.float32)
            weight = loc[pl.ds(a, 1), :] * turned[members + 1 : members + 2]
            high, low = split(turned * weight)
            y16 = y.astype(jnp.bfloat16)
            gram = product(low, y16) + product(high, y16)
            mat = jnp.where(inside, gram[:members], 0.0) + (members - 1.0) * eye
            trace = jnp.sum(
                jnp.sum(mat * eye, axis=0, keepdims=True), axis=1, keepdims=True
            )
            side[a, 0:1, :] = gram[members : members + 1, :]
            side[a, 1:2, :] = jnp.broadcast_to(trace, (1, LANES))
            start = mat / trace
            corr = 1.5 * eye - 0.5 * start
            right = as_right(corr)
            zl[a], zr[a] = as_left(corr), right
            root = product(as_left(start), right)
            rl[a], rr[a] = as_left(root), as_right(root)
        return carry

    lax.fori_loop(0, group // batch, begin, 0)

    def newton(i, carry):
        for a in range(group):
            corr = 1.5 * eye - 0.5 * product(zl[a], rr[a])
            ml[a], mr[a] = as_left(corr), as_right(corr)
        for a in range(group):
            root = product(rl[a], mr[a])
            inverse = product(ml[a], zr[a])
            rl[a], rr[a] = as_left(root), as_right(root)
            zl[a], zr[a] = as_left(inverse), as_right(inverse)
        return carry

    lax.fori_loop(0, ITERS - 2, newton, 0)
    lane = iota2((2 * HALF, LANES), 1)
    row8 = iota2((8, LANES), 0)

    def finish(i, carry):
        for k in range(batch):
            a = i * batch + k
            corr = 1.5 * eye - 0.5 * product(zl[a], rr[a])
            inverse = product(as_left(corr), zr[a])
            trace = side[a, 1:2, :]
            half_way = jnp.sum(
                jnp.where(inside, inverse * side[a, 0:1, :], 0.0), axis=1, keepdims=True
            )
            mean_weight = jnp.sum(inverse * half_way, axis=0, keepdims=True) / trace
            spread = inverse * jnp.sqrt((members - 1.0) / trace)
            body = jnp.where(lane < 80, spread[48:80], pltpu.roll(spread[16:48], 80, 1))
            corner = pltpu.roll(spread[0:16], 64, 1)
            mean_rows = jnp.broadcast_to(mean_weight, (8, LANES))
            moved = jnp.zeros((8, LANES), jnp.float32)
            for p in range(5):
                moved = jnp.where(row8 == p, pltpu.roll(mean_rows, 112 - 16 * p, 1), moved)
            lane_top = lane[:HALF]
            top = jnp.where((lane_top >= 64) & (lane_top < 80), corner, body[:HALF])
            mean_top = jnp.where((lane[:8] >= 112) & (row8 < 5), moved, top[:8])
            top = jnp.concatenate([mean_top, top[8:]], axis=0)
            packed[pl.ds(a, HALF, stride=2 * group), :] = top
            packed[pl.ds(group + a, HALF, stride=2 * group), :] = body[HALF:]
        return carry

    lax.fori_loop(0, group // batch, finish, 0)
    out[...] = packed[...].astype(jnp.bfloat16)


def transforms(lists, loc, left, own, right, members):
    group, local = loc.shape
    lists = lists.reshape(-1)
    tile = own.shape[0]
    f32, b16 = jnp.float32, jnp.bfloat16
    vmem = pl.BlockSpec(memory_space=pltpu.VMEM)
    low_high = pltpu.VMEM((group, members, 2 * LANES), b16)
    stacked = pltpu.VMEM((group, 2 * LANES, LANES), b16)
    return pl.pallas_call(
        transform_body,
        out_shape=pltpu.VMEM((HALF * 2 * group, LANES), b16),
        in_specs=[pl.BlockSpec(memory_space=pltpu.SMEM), vmem, vmem, vmem, vmem],
        out_specs=vmem,
        scratch_shapes=[
            pltpu.VMEM((3 * tile, LANES), f32),
            pltpu.VMEM((group * local, LANES), f32),
            low_high,
            stacked,
            low_high,
            stacked,
            low_high,
            stacked,
            pltpu.VMEM((group, 8, LANES), f32),
            pltpu.VMEM((HALF * 2 * group, LANES), f32),
        ],
        name="transforms",
    )(lists, in_vmem(loc), in_vmem(left), in_vmem(own), in_vmem(right))


def deviation_body(ens, dev, mean, ens32):
    members, step = ens.shape[0], ens.shape[1]
    wide = ens[...].astype(jnp.float32)
    center = jnp.sum(wide, axis=0) * (1.0 / members)
    first = pl.program_id(0) * step
    mean[pl.ds(pl.multiple_of(first, step), step), :] = center
    ens32[...] = (wide - center[None]).reshape(members * step, LANES)
    for o in range(step):
        dev[first + o] = ens32[pl.ds(o, members, stride=step), :].astype(jnp.bfloat16)


def deviations(ensemble):
    members, blocks, cells = ensemble.shape
    step = 48
    whole = pl.BlockSpec(memory_space=pltpu.VMEM)
    return pl.pallas_call(
        deviation_body,
        grid=(blocks // step,),
        out_shape=(
            pltpu.VMEM((blocks, members, cells), jnp.bfloat16),
            pltpu.VMEM((blocks, cells), jnp.float32),
        ),
        in_specs=[pl.BlockSpec((members, step, cells), lambda i: (0, i, 0))],
        out_specs=(whole, whole),
        scratch_shapes=[pltpu.VMEM((members * step, LANES), jnp.float32)],
        name="deviations",
    )(ensemble)


def apply_body(pieces, dev, mean, out, mix32, mix32b, out32):
    members, blocks = out.shape[0], out.shape[1]
    begin = pl.program_id(0) * blocks
    begin = pl.multiple_of(begin, blocks)
    other = pl.multiple_of(begin + dev.shape[0], blocks)
    for ref, at in ((mix32, begin), (mix32b, other)):
        part = pieces[:, pl.ds(at, blocks), :]
        ref[...] = part.astype(jnp.float32).reshape(16 * blocks, LANES)
    centers = mean[pl.ds(begin, blocks), :]
    lane = iota2((16, LANES), 1)
    row = iota2((16, LANES), 0)
    lane8, row8 = lane[:8], row[:8]
    zero = jnp.zeros((16, LANES), jnp.float32)
    none = jnp.zeros((16, LANES), jnp.bfloat16)
    keep = lambda low, high, x: jnp.where((lane >= low) & (lane < high), x, 0.0)

    for g in range(blocks // 4):
        packs = []
        for k in range(4):
            packs.append(mix32[pl.ds(4 * g + k, 16, stride=blocks), :])
            packs.append(mix32b[pl.ds(4 * g + k, 16, stride=blocks), :])
        flip = jnp.transpose(jnp.concatenate(packs, axis=0))
        for k in range(4):
            o = 4 * g + k
            first, second = packs[2 * k], packs[2 * k + 1]
            at = 32 * k
            inner_at = (32, 0, 32, 0)[k]
            corner_at = (64, 64, 96, 64)[k]
            inner = pltpu.roll(flip[80:112], (inner_at - at) % LANES, 1)
            corner = pltpu.roll(first, 32, 1) if corner_at == 96 else first
            means = pltpu.roll(first[:8], 16, 1, stride=16, stride_axis=0)
            means = jnp.where((lane8 // 16 == row8) & (row8 < 5), means, 0.0)
            means = jnp.sum(means, axis=0, keepdims=True)
            means = jnp.where(row == 0, jnp.broadcast_to(means, row.shape), 0.0)
            direct = [
                zero,
                keep(80, 112, first),
                keep(80, 128, second[:16]),
                keep(0, 64, first),
                keep(0, 80, second),
                means,
            ]
            turned = [
                keep(at, at + 32, flip[0:16])
                + keep(inner_at, inner_at + 32, inner[:16])
                + keep(corner_at, corner_at + 16, corner),
                keep(at, at + 32, flip[16:32]) + keep(inner_at + 16, inner_at + 32, inner[16:]),
                keep(at, at + 32, flip[32:48]),
                keep(at + 16, at + 32, flip[48:64]),
                zero,
                zero,
            ]
            weights = jnp.concatenate(
                [
                    jnp.concatenate(direct, axis=0).astype(jnp.bfloat16),
                    jnp.concatenate(turned, axis=0).astype(jnp.bfloat16),
                ],
                axis=1,
            )
            d = dev[begin + o]
            outer, middle, start = d[48:80], d[16:48], d[0:16]
            tail = (
                [outer, middle, start, none, none, none],
                [middle, outer, start, none, none, none],
                [none, none, middle, outer, start, none],
                [middle, none, none, start, none, outer],
            )[k]
            source = jnp.concatenate([d, d[:48]] + tail, axis=0)
            result = jnp.dot(weights, source, preferred_element_type=jnp.float32)
            base = centers[o : o + 1, :] + result[members : members + 1]
            out32[pl.ds(o, members, stride=blocks), :] = result[:members] + base
    out[...] = out32[...].reshape(members, blocks, LANES).astype(jnp.bfloat16)


def apply_weights(pieces, dev, mean):
    blocks, members, cells = dev.shape
    step = 48
    f32 = jnp.float32
    return pl.pallas_call(
        apply_body,
        grid=(blocks // step,),
        out_shape=jax.ShapeDtypeStruct((members, blocks, cells), jnp.bfloat16),
        in_specs=[pl.BlockSpec(memory_space=pltpu.VMEM)] * 3,
        out_specs=pl.BlockSpec((members, step, cells), lambda i: (0, i, 0)),
        scratch_shapes=[
            pltpu.VMEM((16 * step, LANES), f32),
            pltpu.VMEM((16 * step, LANES), f32),
            pltpu.VMEM((members * step, LANES), f32),
        ],
        name="apply",
    )(in_vmem(pieces), in_vmem(dev), in_vmem(mean))


def shards(
    obs_pert,
    innovation,
    obs_prec,
    obs_lists,
    loc_weight,
    send_rows,
    ocean_src,
    ocean_frac,
    ocean_ens,
):
    n_member = lax.axis_size("member")
    n_space = lax.axis_size("space")
    member_idx = lax.axis_index("member")
    own_members, tile_obs = obs_pert.shape
    members = own_members * n_member
    chunks = tile_obs // LANES
    b16 = jnp.bfloat16

    flat = obs_pert.reshape(own_members * chunks, LANES)
    spread = lax.all_to_all(
        jnp.broadcast_to(flat[None], (n_member, *flat.shape)), "member", 0, 0, tiled=True
    )
    spread, innovation, obs_prec, obs_lists, loc_weight, send_rows, ocean_ens = (
        lax.optimization_barrier(
            (spread, innovation, obs_prec, obs_lists, loc_weight, send_rows, ocean_ens)
        )
    )
    by_obs = spread.reshape(n_member, own_members, chunks, LANES).transpose(2, 3, 0, 1)
    by_obs = by_obs.reshape(tile_obs, members)
    own = jnp.concatenate(
        [
            by_obs,
            innovation[:, None],
            obs_prec[:, None],
            jnp.zeros((tile_obs, LANES - members - 2), b16),
        ],
        axis=1,
    )
    left = lax.ppermute(own, "space", [(i, (i + 1) % n_space) for i in range(n_space)])
    right = lax.ppermute(own, "space", [((i + 1) % n_space, i) for i in range(n_space)])

    group = obs_lists.shape[0] // n_member
    lists_mine = lax.dynamic_slice_in_dim(obs_lists, member_idx * group, group, 0)
    loc_mine = lax.dynamic_slice_in_dim(loc_weight, member_idx * group, group, 0)
    loc_mine = loc_mine.astype(jnp.float32)
    count = 2 * n_member
    home = jnp.arange(n_member, dtype=jnp.int32)[:, None] * (2 * group)
    choice = (send_rows[0] + home).T
    choice = jnp.concatenate([choice, choice + group], axis=1).reshape(-1)
    dev, mean = deviations(ocean_ens)
    lists_mine, loc_mine, left, own, right, choice, dev, mean = lax.optimization_barrier(
        (lists_mine, loc_mine, left, own, right, choice, dev, mean)
    )
    pieces = transforms(lists_mine, loc_mine, left, own, right, members)

    arrived_one = lax.all_to_all(
        pieces.reshape(n_member, 2 * group, LANES), "member", 0, 0, tiled=True
    ).reshape(n_member * 2 * group, LANES)
    arrived_one, ocean_src, ocean_frac = lax.optimization_barrier(
        (arrived_one, ocean_src, ocean_frac)
    )
    places = jnp.arange(n_member * 2 * group, dtype=jnp.int32)[None]
    pick = (choice[:, None] == places).astype(b16)
    chosen = jnp.dot(pick, arrived_one, preferred_element_type=jnp.float32).astype(b16)
    arrived = lax.all_to_all(
        chosen.reshape(n_space, count, LANES), "space", 0, 0, tiled=True
    ).reshape(n_space * count, LANES)
    slot = (ocean_src % n_space) * count + ocean_src // n_space
    slot = jnp.concatenate([slot, slot + n_member], axis=0)
    frac = jnp.concatenate([ocean_frac, ocean_frac])[:, None]
    places = jnp.arange(n_space * count, dtype=jnp.int32)[None]
    coef = jnp.where(slot[:, :1] == places, 1.0 - frac, 0.0) + jnp.where(
        slot[:, 1:] == places, frac, 0.0
    )
    halves = jnp.dot(
        coef, arrived.astype(jnp.float32), precision=lax.Precision.HIGHEST
    ).astype(b16)
    everything = lax.all_gather(halves, "member", axis=0, tiled=True)
    return apply_weights(everything.reshape(n_member, *halves.shape), dev, mean)


def solution(mesh):
    return jax.shard_map(
        shards,
        mesh=mesh,
        in_specs=(
            P("member", "space"),
            P("space"),
            P("space"),
            P("space", None),
            P("space", None),
            P("space", None, None),
            P("space", None),
            P("space"),
            P(None, "space", "member"),
        ),
        out_specs=P(None, "space", "member"),
        check_vma=False,
    )
```

```python
import jax
import jax.numpy as jnp
from jax import lax
from jax.experimental import pallas as pl
from jax.experimental.pallas import tpu as pltpu
from jax.sharding import PartitionSpec as P

ITERS = 12
LANES = 128
HALF = 16


def in_vmem(x):
    return pltpu.with_memory_space_constraint(x, pltpu.VMEM)


def iota2(shape, dim):
    return lax.broadcasted_iota(jnp.int32, shape, dim)


def split(x):
    high = x.astype(jnp.bfloat16)
    low = (x - high.astype(jnp.float32)).astype(jnp.bfloat16)
    return high, low


def as_left(high, low):
    lane = iota2(high.shape, 1)
    low = pltpu.roll(low, 80, 1)
    again = pltpu.roll(high, 32, 1)
    first = jnp.where(lane < 80, high, low)
    second = jnp.where(lane < 32, low, again)
    return jnp.concatenate([first, second], axis=1)


def as_right(high, low):
    none = jnp.zeros((16, high.shape[1]), jnp.bfloat16)
    return jnp.concatenate([high, high, low, none], axis=0)


def both(x):
    parts = split(x)
    return as_left(*parts), as_right(*parts)


def product(left, right):
    return jnp.dot(left, right, preferred_element_type=jnp.float32)


def transform_body(
    lists, loc, left, own, right, out, table, rows, rl, rr, zl, zr, ml, mr, side, packed
):
    group, local = loc.shape
    tile = own.shape[0]
    members = rl.shape[1]
    for i, part in enumerate((left, own, right)):
        table[pl.ds(i * tile, tile), :] = part[...].astype(jnp.float32)
    eye = (iota2((members, LANES), 0) == iota2((members, LANES), 1)).astype(jnp.float32)
    inside = iota2((members, LANES), 1) < members
    step = 32
    batch = 4

    def pull(i, carry):
        for u in range(step):
            spot = lists[i * step + u]
            rows[pl.ds(i * step + u, 1), :] = table[pl.ds(spot, 1), :]
        return carry

    lax.fori_loop(0, group * local // step, pull, 0)

    def begin(i, carry):
        for k in range(batch):
            a = i * batch + k
            y = rows[pl.ds(a * local, local), :]
            turned = jnp.transpose(y.astype(jnp.bfloat16))[:96].astype(jnp.float32)
            weight = loc[pl.ds(a, 1), :] * turned[members + 1 : members + 2]
            high, low = split(turned * weight)
            y16 = y.astype(jnp.bfloat16)
            gram = product(low, y16) + product(high, y16)
            mat = jnp.where(inside, gram[:members], 0.0) + (members - 1.0) * eye
            trace = jnp.sum(
                jnp.sum(mat * eye, axis=0, keepdims=True), axis=1, keepdims=True
            )
            side[a, 0:1, :] = gram[members : members + 1, :]
            side[a, 1:2, :] = jnp.broadcast_to(trace, (1, LANES))
            start = mat * (0.5 / trace)
            zl[a], zr[a] = both(1.5 * eye - start)
            rl[a], rr[a] = both(product(as_left(*split(start)), zr[a]))
        return carry

    lax.fori_loop(0, group // batch, begin, 0)

    def newton(i, carry):
        for a in range(group):
            ml[a], mr[a] = both(1.5 * eye - product(zl[a], rr[a]))
        for a in range(group):
            rl[a], rr[a] = both(product(rl[a], mr[a]))
            zl[a], zr[a] = both(product(ml[a], zr[a]))
        return carry

    lax.fori_loop(0, ITERS - 2, newton, 0)
    lane = iota2((2 * HALF, LANES), 1)
    row8 = iota2((8, LANES), 0)

    def finish(i, carry):
        for k in range(batch):
            a = i * batch + k
            corr = 1.5 * eye - product(zl[a], rr[a])
            inverse = product(as_left(*split(corr)), zr[a])
            trace = side[a, 1:2, :]
            half_way = jnp.sum(
                jnp.where(inside, inverse * side[a, 0:1, :], 0.0), axis=1, keepdims=True
            )
            mean_weight = jnp.sum(inverse * half_way, axis=0, keepdims=True) / trace
            spread = inverse * jnp.sqrt((members - 1.0) / trace)
            body = jnp.where(lane < 80, spread[48:80], pltpu.roll(spread[16:48], 80, 1))
            corner = pltpu.roll(spread[0:16], 64, 1)
            mean_rows = jnp.broadcast_to(mean_weight, (8, LANES))
            moved = jnp.zeros((8, LANES), jnp.float32)
            for p in range(5):
                moved = jnp.where(row8 == p, pltpu.roll(mean_rows, 112 - 16 * p, 1), moved)
            lane_top = lane[:HALF]
            top = jnp.where((lane_top >= 64) & (lane_top < 80), corner, body[:HALF])
            mean_top = jnp.where((lane[:8] >= 112) & (row8 < 5), moved, top[:8])
            top = jnp.concatenate([mean_top, top[8:]], axis=0)
            packed[pl.ds(a, HALF, stride=2 * group), :] = top
            packed[pl.ds(group + a, HALF, stride=2 * group), :] = body[HALF:]
        return carry

    lax.fori_loop(0, group // batch, finish, 0)
    out[...] = packed[...].astype(jnp.bfloat16)


def transforms(lists, loc, left, own, right, members):
    group, local = loc.shape
    tile = own.shape[0]
    f32, b16 = jnp.float32, jnp.bfloat16
    vmem = pl.BlockSpec(memory_space=pltpu.VMEM)
    low_high = pltpu.VMEM((group, members, 2 * LANES), b16)
    stacked = pltpu.VMEM((group, 2 * LANES, LANES), b16)
    return pl.pallas_call(
        transform_body,
        out_shape=pltpu.VMEM((HALF * 2 * group, LANES), b16),
        in_specs=[pl.BlockSpec(memory_space=pltpu.SMEM), vmem, vmem, vmem, vmem],
        out_specs=vmem,
        scratch_shapes=[
            pltpu.VMEM((3 * tile, LANES), f32),
            pltpu.VMEM((group * local, LANES), f32),
            low_high,
            stacked,
            low_high,
            stacked,
            low_high,
            stacked,
            pltpu.VMEM((group, 8, LANES), f32),
            pltpu.VMEM((HALF * 2 * group, LANES), f32),
        ],
        name="transforms",
    )(lists, in_vmem(loc), in_vmem(left), in_vmem(own), in_vmem(right))


def spread_body(pert, out, flat):
    wide = pert[...].astype(jnp.float32)
    count, tile = wide.shape
    for c in range(tile // LANES):
        flat[c * count : (c + 1) * count, :] = wide[:, c * LANES : (c + 1) * LANES]
    rows = flat[...].astype(jnp.bfloat16)
    for p in range(out.shape[0]):
        out[p] = rows


def copies(pert, devices):
    count, tile = pert.shape
    shape = (count * tile // LANES, LANES)
    vmem = pl.BlockSpec(memory_space=pltpu.VMEM)
    return pl.pallas_call(
        spread_body,
        out_shape=pltpu.VMEM((devices, *shape), jnp.bfloat16),
        in_specs=[vmem],
        out_specs=vmem,
        scratch_shapes=[pltpu.VMEM(shape, jnp.float32)],
        name="copies",
    )(pert)


def deviation_body(ens, dev, mean, ens32):
    members, step = ens.shape[0], ens.shape[1]
    wide = ens[...].astype(jnp.float32)
    center = jnp.sum(wide, axis=0) * (1.0 / members)
    first = pl.program_id(0) * step
    mean[pl.ds(pl.multiple_of(first, step), step), :] = center
    ens32[...] = (wide - center[None]).reshape(members * step, LANES)
    for o in range(step):
        dev[first + o] = ens32[pl.ds(o, members, stride=step), :].astype(jnp.bfloat16)


def deviations(ensemble):
    members, blocks, cells = ensemble.shape
    step = 48
    whole = pl.BlockSpec(memory_space=pltpu.VMEM)
    return pl.pallas_call(
        deviation_body,
        grid=(blocks // step,),
        out_shape=(
            pltpu.VMEM((blocks, members, cells), jnp.bfloat16),
            pltpu.VMEM((blocks, cells), jnp.float32),
        ),
        in_specs=[pl.BlockSpec((members, step, cells), lambda i: (0, i, 0))],
        out_specs=(whole, whole),
        scratch_shapes=[pltpu.VMEM((members * step, LANES), jnp.float32)],
        name="deviations",
    )(ensemble)


def apply_body(pieces, dev, mean, out, mix32, mix32b, out32):
    members, blocks = out.shape[0], out.shape[1]
    begin = pl.program_id(0) * blocks
    begin = pl.multiple_of(begin, blocks)
    other = pl.multiple_of(begin + dev.shape[0], blocks)
    for ref, at in ((mix32, begin), (mix32b, other)):
        part = pieces[:, pl.ds(at, blocks), :]
        ref[...] = part.astype(jnp.float32).reshape(16 * blocks, LANES)
    centers = mean[pl.ds(begin, blocks), :]
    lane = iota2((16, LANES), 1)
    row = iota2((16, LANES), 0)
    lane8, row8 = lane[:8], row[:8]
    zero = jnp.zeros((16, LANES), jnp.float32)
    none = jnp.zeros((16, LANES), jnp.bfloat16)
    keep = lambda low, high, x: jnp.where((lane >= low) & (lane < high), x, 0.0)

    for g in range(blocks // 4):
        packs = []
        for k in range(4):
            packs.append(mix32[pl.ds(4 * g + k, 16, stride=blocks), :])
            packs.append(mix32b[pl.ds(4 * g + k, 16, stride=blocks), :])
        flip = jnp.transpose(jnp.concatenate(packs, axis=0))
        for k in range(4):
            o = 4 * g + k
            first, second = packs[2 * k], packs[2 * k + 1]
            at = 32 * k
            inner_at = (32, 0, 32, 0)[k]
            corner_at = (64, 64, 96, 64)[k]
            inner = pltpu.roll(flip[80:112], (inner_at - at) % LANES, 1)
            corner = pltpu.roll(first, 32, 1) if corner_at == 96 else first
            means = pltpu.roll(first[:8], 16, 1, stride=16, stride_axis=0)
            means = jnp.where((lane8 // 16 == row8) & (row8 < 5), means, 0.0)
            means = jnp.sum(means, axis=0, keepdims=True)
            means = jnp.where(row == 0, jnp.broadcast_to(means, row.shape), 0.0)
            direct = [
                zero,
                keep(80, 112, first),
                keep(80, 128, second[:16]),
                keep(0, 64, first),
                keep(0, 80, second),
                means,
            ]
            turned = [
                keep(at, at + 32, flip[0:16])
                + keep(inner_at, inner_at + 32, inner[:16])
                + keep(corner_at, corner_at + 16, corner),
                keep(at, at + 32, flip[16:32]) + keep(inner_at + 16, inner_at + 32, inner[16:]),
                keep(at, at + 32, flip[32:48]),
                keep(at + 16, at + 32, flip[48:64]),
                zero,
                zero,
            ]
            weights = jnp.concatenate(
                [
                    jnp.concatenate(direct, axis=0).astype(jnp.bfloat16),
                    jnp.concatenate(turned, axis=0).astype(jnp.bfloat16),
                ],
                axis=1,
            )
            d = dev[begin + o]
            outer, middle, start = d[48:80], d[16:48], d[0:16]
            tail = (
                [outer, middle, start, none, none, none],
                [middle, outer, start, none, none, none],
                [none, none, middle, outer, start, none],
                [middle, none, none, start, none, outer],
            )[k]
            source = jnp.concatenate([d, d[:48]] + tail, axis=0)
            result = jnp.dot(weights, source, preferred_element_type=jnp.float32)
            base = centers[o : o + 1, :] + result[members : members + 1]
            out32[pl.ds(o, members, stride=blocks), :] = result[:members] + base
    out[...] = out32[...].reshape(members, blocks, LANES).astype(jnp.bfloat16)


def apply_weights(pieces, dev, mean):
    blocks, members, cells = dev.shape
    step = 48
    f32 = jnp.float32
    return pl.pallas_call(
        apply_body,
        grid=(blocks // step,),
        out_shape=jax.ShapeDtypeStruct((members, blocks, cells), jnp.bfloat16),
        in_specs=[pl.BlockSpec(memory_space=pltpu.VMEM)] * 3,
        out_specs=pl.BlockSpec((members, step, cells), lambda i: (0, i, 0)),
        scratch_shapes=[
            pltpu.VMEM((16 * step, LANES), f32),
            pltpu.VMEM((16 * step, LANES), f32),
            pltpu.VMEM((members * step, LANES), f32),
        ],
        name="apply",
    )(in_vmem(pieces), in_vmem(dev), in_vmem(mean))


def shards(
    obs_pert,
    innovation,
    obs_prec,
    obs_lists,
    loc_weight,
    send_rows,
    ocean_src,
    ocean_frac,
    ocean_ens,
):
    n_member = lax.axis_size("member")
    n_space = lax.axis_size("space")
    member_idx = lax.axis_index("member")
    own_members, tile_obs = obs_pert.shape
    members = own_members * n_member
    chunks = tile_obs // LANES
    b16 = jnp.bfloat16

    spread = lax.all_to_all(copies(obs_pert, n_member), "member", 0, 0, tiled=True)
    spread, obs_lists, loc_weight, send_rows, ocean_ens = lax.optimization_barrier(
        (spread, obs_lists, loc_weight, send_rows, ocean_ens)
    )
    by_obs = spread.reshape(n_member, chunks, own_members, LANES).transpose(1, 3, 0, 2)
    by_obs = by_obs.reshape(tile_obs, members)
    own = jnp.concatenate(
        [
            by_obs,
            innovation[:, None],
            obs_prec[:, None],
            jnp.zeros((tile_obs, LANES - members - 2), b16),
        ],
        axis=1,
    )
    left = lax.ppermute(own, "space", [(i, (i + 1) % n_space) for i in range(n_space)])
    right = lax.ppermute(own, "space", [((i + 1) % n_space, i) for i in range(n_space)])

    group = obs_lists.shape[0] // n_member
    lists_mine = lax.dynamic_slice_in_dim(obs_lists, member_idx * group, group, 0).reshape(-1)
    loc_mine = lax.dynamic_slice_in_dim(loc_weight, member_idx * group, group, 0)
    loc_mine = loc_mine.astype(jnp.float32)
    count = 2 * n_member
    home = jnp.arange(n_member, dtype=jnp.int32)[:, None] * (2 * group)
    choice = (send_rows[0] + home).T
    choice = jnp.concatenate([choice, choice + group], axis=1).reshape(-1)
    dev, mean = deviations(ocean_ens)
    lists_mine, loc_mine, left, own, right, choice, dev, mean = lax.optimization_barrier(
        (lists_mine, loc_mine, left, own, right, choice, dev, mean)
    )
    pieces = transforms(lists_mine, loc_mine, left, own, right, members)

    arrived_one = lax.all_to_all(
        pieces.reshape(n_member, 2 * group, LANES), "member", 0, 0, tiled=True
    ).reshape(n_member * 2 * group, LANES)
    arrived_one, ocean_src, ocean_frac = lax.optimization_barrier(
        (arrived_one, ocean_src, ocean_frac)
    )
    places = jnp.arange(n_member * 2 * group, dtype=jnp.int32)[None]
    pick = (choice[:, None] == places).astype(b16)
    chosen = jnp.dot(pick, arrived_one, preferred_element_type=jnp.float32).astype(b16)
    arrived = lax.all_to_all(
        chosen.reshape(n_space, count, LANES), "space", 0, 0, tiled=True
    ).reshape(n_space * count, LANES)
    slot = (ocean_src % n_space) * count + ocean_src // n_space
    slot = jnp.concatenate([slot, slot + n_member], axis=0)
    frac = jnp.concatenate([ocean_frac, ocean_frac])[:, None]
    places = jnp.arange(n_space * count, dtype=jnp.int32)[None]
    coef = jnp.where(slot[:, :1] == places, 1.0 - frac, 0.0) + jnp.where(
        slot[:, 1:] == places, frac, 0.0
    )
    halves = jnp.dot(
        coef, arrived.astype(jnp.float32), precision=lax.Precision.HIGHEST
    ).astype(b16)
    everything = lax.all_gather(halves, "member", axis=0, tiled=True)
    return apply_weights(everything.reshape(n_member, *halves.shape), dev, mean)


def solution(mesh):
    return jax.shard_map(
        shards,
        mesh=mesh,
        in_specs=(
            P("member", "space"),
            P("space"),
            P("space"),
            P("space", None),
            P("space", None),
            P("space", None, None),
            P("space", None),
            P("space"),
            P(None, "space", "member"),
        ),
        out_specs=P(None, "space", "member"),
        check_vma=False,
    )
```
